32 devices in a mesh: tp: 2 (over x), dp: 4 (over y, core), rep: 4 (over z).
Axes of the slice: x: 2, y: 2, z: 4, core: 2. Of those that a mesh axis runs over, the one named last changes fastest.
Arguments:
- prompts: bfloat16 [12288, 8192], P(('dp', 'rep'), 'tp'), may hold values from -6 to 6
- frozen_projection_weight: bfloat16 [2, 8192, 2048], P(None, ('dp', 'rep'), 'tp'), may hold values from -5 to 5
- lowrank_down_factor: bfloat16 [2, 8192, 64], P(None, ('dp', 'rep')), may hold values from -0.119628906 to 0.119628906
- lowrank_up_factor: bfloat16 [2, 64, 2048], P(None, None, 'tp'), may hold values from -0.59765625 to 0.59765625
- magnitude: float32 [2, 2048], P(None, 'tp'), may hold values from 0.5 to 2
Outputs:
- key_values: bfloat16 [2, 12288, 2048], P(None, ('dp', 'rep'), 'tp')
The draws below stay inside these ranges and needn't reach their ends.
All inputs are finite; a program needn't handle non-finite values.
Results may differ from the reference program's by a relative error of at most 0.0049.
Values may be sent and summed in bfloat16 or wider, within the bound.
A program may use at most 128 MiB of HBM per device.

```python
import math
import jax
import jax.numpy as jnp
from jax import lax

MODEL_WIDTH = 8192
LOWRANK_SIZE = 64
LAYER_COUNT = 2
PROJECTION_COLUMNS = 2048
TOKENS = 12288


def draw_frozen_projection_weight(key, part):
    streams = jax.random.split(jax.random.fold_in(key, 17), 3)
    position = jnp.arange(MODEL_WIDTH, dtype=jnp.float32)[None, :, None] / MODEL_WIDTH
    row_rough = jnp.exp(jax.random.uniform(streams[1], (LAYER_COUNT, MODEL_WIDTH, 1), jnp.float32, -1.2, 1.2))
    col_rough = jnp.exp(jax.random.uniform(streams[2], (LAYER_COUNT, 1, PROJECTION_COLUMNS), jnp.float32, -1.2, 1.2))
    noise = jnp.clip(jax.random.normal(streams[0], (LAYER_COUNT, MODEL_WIDTH, PROJECTION_COLUMNS), jnp.float32), -4.0, 4.0)
    ramp = jnp.sqrt(1.0 + 2.0 * position)
    values = noise * row_rough * col_rough * ramp / math.sqrt(MODEL_WIDTH)
    return values.astype(jnp.bfloat16)


def steps_of(key, extent, cuts, low, top_value):
    gain = 1.0
    for dim, shards_of in cuts:
        draws = jax.random.uniform(jax.random.fold_in(jax.random.fold_in(key, 6), dim), (shards_of,), jnp.float32, low / len(cuts), top_value / len(cuts))
        gain = gain * jnp.repeat(jnp.exp(draws), extent[dim] // shards_of).reshape((-1,) + (1,) * (len(extent) - 1 - dim))
    return gain


def gaussian(rng, shape, deviation, reach, shards=(), held_as=jnp.bfloat16):
    values = jax.random.normal(rng, shape, jnp.float32) * deviation
    if len(shards) > 0:
        values = steps_of(rng, shape, shards, -0.22, 0.18) * values
    return jnp.clip(values, min=-reach, max=reach).astype(held_as)


def setup_inputs(seed: int = 0) -> dict:
    keys = jax.random.split(jax.random.key(seed), 6)
    return {
        "prompts": gaussian(keys[0], (TOKENS, MODEL_WIDTH), 1.0, 6.0, ((0, 16), (1, 2))),
        "frozen_projection_weight": draw_frozen_projection_weight(jax.random.fold_in(keys[5], 71), 0),
        "lowrank_down_factor": gaussian(keys[2], (LAYER_COUNT, MODEL_WIDTH, LOWRANK_SIZE), 0.02, 0.119628906, ((1, 16),)),
        "lowrank_up_factor": gaussian(keys[3], (LAYER_COUNT, LOWRANK_SIZE, PROJECTION_COLUMNS), 0.1, 0.59765625, ((2, 2),)),
        "magnitude": jnp.clip(jnp.exp(math.log(2.0) - 1.3862944 * jax.random.uniform(keys[4], (LAYER_COUNT, PROJECTION_COLUMNS), jnp.float32) ** steps_of(keys[4], (LAYER_COUNT, PROJECTION_COLUMNS), ((1, 2),), -0.2, 0.2)), 0.5, 2.0),
    }


epsilon = 1e-06

def reference(prompts, frozen_projection_weight, lowrank_down_factor, lowrank_up_factor, magnitude):
    outputs = []
    for current_layer_index in range(LAYER_COUNT):
        combined_weight = frozen_projection_weight[current_layer_index].astype(jnp.float32) + jnp.dot(lowrank_down_factor[current_layer_index], lowrank_up_factor[current_layer_index], preferred_element_type=jnp.float32)
        norms = jnp.sqrt(lax.optimization_barrier(jnp.sum(combined_weight * combined_weight, axis=0)) + epsilon)
        factor = magnitude[current_layer_index] / norms
        prefilled_key_values = (combined_weight * factor).astype(jnp.bfloat16)
        outputs.append(jnp.dot(prompts, prefilled_key_values, preferred_element_type=jnp.float32).astype(jnp.bfloat16))
    return jnp.stack(outputs)
```

```python
import functools

import jax
import jax.numpy as jnp
from jax import lax
from jax.experimental import pallas as pl
from jax.experimental.pallas import tpu as pltpu
from jax.sharding import PartitionSpec as P

epsilon = 1e-06
MESH = pl.DeviceIdType.MESH


def merge_rows(weight_rows, down_rows, up_matrix):
    return weight_rows.astype(jnp.float32) + jnp.einsum(
        "lrk,lkc->lrc", down_rows, up_matrix, preferred_element_type=jnp.float32
    )


def kernel(
    sizes, prompts_ref, merged_ref, magnitude_ref, out_ref,
    wbuf, pbuf, acc, squares,
    arrive, zsend, zown, ysend, csend, psend, parrive, load_p, load_w,
):
    tp_size, dp_size, rep_size = sizes
    y_size = dp_size // 2
    layers, rows, columns = merged_ref.shape
    groups = dp_size // tp_size
    x = lax.axis_index("tp")
    d = lax.axis_index("dp")
    z = lax.axis_index("rep")
    y, c = d // 2, lax.rem(d, 2)
    partner = {"tp": x, "dp": d + 1 - 2 * c, "rep": z}

    pieces = [(0, 0, rows // 4), (0, rows // 4, rows - rows // 4)]
    for layer in range(1, layers):
        pieces += [(layer, 0, rows // 2), (layer, rows // 2, rows // 2)]
    count = len(pieces)

    def block(yy, cc, zz):
        return (yy * 2 + cc) * rep_size + zz

    def piece(b, s):
        layer, start, size = pieces[s]
        return wbuf.at[b, layer, pl.ds(start, size), :]

    pending = []

    def send(cond, ref, send_sem, recv_sem, device):
        def make():
            return pltpu.make_async_remote_copy(
                src_ref=ref, dst_ref=ref, send_sem=send_sem, recv_sem=recv_sem,
                device_id=device, device_id_type=MESH,
            )

        pending.append((cond, make))
        if cond is None:
            make().start()
        else:
            @pl.when(cond)
            def _():
                make().start()

    def wait_piece(b, s):
        pltpu.make_async_remote_copy(
            src_ref=piece(b, s), dst_ref=piece(b, s), send_sem=csend.at[0],
            recv_sem=arrive.at[b * count + s], device_id=partner, device_id_type=MESH,
        ).wait_recv()

    def z_device(step):
        return {"tp": x, "dp": d, "rep": z + step}

    def y_device(o):
        return {"tp": x, "dp": lax.rem(y + o, y_size) * 2 + c, "rep": z}

    def to_partner(cond, yy, zz, s):
        b = block(yy, c, zz)
        send(cond, piece(b, s), csend.at[(yy * rep_size + zz) * count + s], arrive.at[b * count + s], partner)

    def to_y(cond, zz, s):
        b = block(y, c, zz)
        for o in range(1, y_size):
            send(
                cond, piece(b, s), ysend.at[((o - 1) * rep_size + zz) * count + s],
                arrive.at[b * count + s], y_device(o),
            )

    def along_z(cond, yy, zz, s, step):
        b = block(yy, c, zz)
        send(
            cond, piece(b, s), zsend.at[(yy * rep_size + zz) * count + s],
            arrive.at[b * count + s], z_device(step),
        )

    def start_z(yy, s):
        b = block(yy, c, z)
        send(z < rep_size - 1, piece(b, s), zown.at[yy * count + s], arrive.at[b * count + s], z_device(1))
        along_z(z > 0, yy, z, s, -1)

    def when(cond, body):
        if cond is None:
            body()
        else:
            pl.when(cond)(body)

    me = block(y, c, z)
    load_weight = pltpu.make_async_copy(merged_ref, wbuf.at[me], load_w)
    load_weight.start()

    table = [sorted(range(rep_size), key=lambda k: (abs(k - at), k)) for at in range(rep_size)]

    def nearest(i):
        value = jnp.int32(table[0][i])
        for at in range(1, rep_size):
            value = jnp.where(z == at, jnp.int32(table[at][i]), value)
        return value

    own_chunks = []
    for i in range(rep_size):
        for g in range(groups):
            own_chunks.append((g * rep_size + nearest(i), x * groups * rep_size + g * rep_size + nearest(i)))

    def load_chunk(j, b):
        start = pl.multiple_of(j * rows, rows)
        return pltpu.make_async_copy(prompts_ref.at[:, pl.ds(start, rows)], pbuf.at[b], load_p.at[b])

    for j, b in own_chunks:
        load_chunk(j, b).start()

    barrier = pltpu.get_barrier_semaphore()
    pl.semaphore_signal(barrier, 1, device_id=partner, device_id_type=MESH)
    for o in range(1, y_size):
        pl.semaphore_signal(barrier, 1, device_id=y_device(o), device_id_type=MESH)
    for o in range(1, tp_size):
        pl.semaphore_signal(
            barrier, 1, device_id={"tp": lax.rem(x + o, tp_size), "dp": d, "rep": z}, device_id_type=MESH
        )

    @pl.when(z > 0)
    def _():
        pl.semaphore_signal(barrier, 1, device_id=z_device(-1), device_id_type=MESH)

    @pl.when(z < rep_size - 1)
    def _():
        pl.semaphore_signal(barrier, 1, device_id=z_device(1), device_id_type=MESH)

    neighbours = jnp.where(z > 0, 1, 0) + jnp.where(z < rep_size - 1, 1, 0)
    pl.semaphore_wait(barrier, neighbours + (1 + y_size - 1 + tp_size - 1))

    load_weight.wait()
    for s in range(count):
        to_y(None, z, s)
        start_z(y, s)
    for j, b in own_chunks:
        load_chunk(j, b).wait()
        for o in range(1, tp_size):
            send(
                None, pbuf.at[b], psend.at[(o - 1) * dp_size * rep_size + b], parrive.at[b],
                {"tp": lax.rem(x + o, tp_size), "dp": d, "rep": z},
            )
    for s in range(count):
        to_partner(None, y, z, s)

    acc[...] = jnp.zeros_like(acc)
    squares[...] = jnp.zeros_like(squares)
    tile = min(256, columns)

    def wait_chunk(b):
        @pl.when(b // (groups * rep_size) != x)
        def _():
            pltpu.make_async_remote_copy(
                src_ref=pbuf.at[b], dst_ref=pbuf.at[b], send_sem=psend.at[0], recv_sem=parrive.at[b],
                device_id=partner, device_id_type=MESH,
            ).wait_recv()

    def compute(b, first, last):
        tiles = columns // tile

        def step(t, carry):
            layer = first + t // tiles
            at = pl.ds(pl.multiple_of(lax.rem(t, tiles) * tile, tile), tile)
            weight = wbuf[b, layer, :, at]
            acc[layer, :, at] += jnp.dot(pbuf[b], weight, preferred_element_type=jnp.float32)
            wide = weight.astype(jnp.float32)
            squares[layer, :, at] += jnp.sum((wide * wide).reshape(rows // 8, 8, tile), axis=0)
            return carry

        lax.fori_loop(0, (last - first) * tiles, step, 0)

    def finish(zz):
        mine, other = block(y, c, zz), block(y, 1 - c, zz)
        wait_chunk(mine)
        compute(mine, 0, layers)
        for s in range(count):
            wait_piece(other, s)
        wait_chunk(other)
        compute(other, 0, layers)
        for o in range(1, y_size):
            yy = lax.rem(y + o, y_size)
            mine, other = block(yy, c, zz), block(yy, 1 - c, zz)
            for layer in range(layers):
                held = [s for s in range(count) if pieces[s][0] == layer]
                for s in held:
                    if s > 0:
                        wait_piece(mine, s)
                        to_partner_plain(yy, zz, s)
                if layer == 0:
                    wait_chunk(mine)
                compute(mine, layer, layer + 1)
                for s in held:
                    wait_piece(other, s)
                if layer == 0:
                    wait_chunk(other)
                compute(other, layer, layer + 1)

    def to_partner_plain(yy, zz, s):
        b = block(yy, c, zz)

        def make():
            return pltpu.make_async_remote_copy(
                src_ref=piece(b, s), dst_ref=piece(b, s), send_sem=csend.at[(yy * rep_size + zz) * count + s],
                recv_sem=arrive.at[b * count + s], device_id=partner, device_id_type=MESH,
            )

        make().start()

    def take(zz, s, step):
        onward = (z + step >= 0) & (z + step <= rep_size - 1)

        def arrived(yy):
            b = block(yy, c, zz)
            wait_piece(b, s)

            @pl.when(onward)
            def _():
                pltpu.make_async_remote_copy(
                    src_ref=piece(b, s), dst_ref=piece(b, s), send_sem=zsend.at[(yy * rep_size + zz) * count + s],
                    recv_sem=arrive.at[b * count + s], device_id=z_device(step), device_id_type=MESH,
                ).start()

        arrived(y)
        if s > 0:
            b = block(y, c, zz)
            for o in range(1, y_size):
                pltpu.make_async_remote_copy(
                    src_ref=piece(b, s), dst_ref=piece(b, s),
                    send_sem=ysend.at[((o - 1) * rep_size + zz) * count + s],
                    recv_sem=arrive.at[b * count + s], device_id=y_device(o), device_id_type=MESH,
                ).start()
        to_partner_plain(y, zz, s)
        if s == 0:
            for o in range(1, y_size):
                yy = lax.rem(y + o, y_size)
                arrived(yy)
                to_partner_plain(yy, zz, 0)

    for o in range(1, y_size):
        yy = lax.rem(y + o, y_size)
        wait_piece(block(yy, c, z), 0)
        start_z(yy, 0)
        to_partner(None, yy, z, 0)

    def sides(r):
        return ((z - r >= 0, z - r, 1), (z + r <= rep_size - 1, z + r, -1))

    for r in range(1, rep_size):
        for s in range(count):
            for valid, zz, step in sides(r):
                pl.when(valid)(functools.partial(take, zz, s, step))
        if r == 1:
            finish(z)
        else:
            for valid, zz, _ in sides(r - 1):
                pl.when(valid)(functools.partial(finish, zz))
    if rep_size == 1:
        finish(z)
    else:
        for valid, zz, _ in sides(rep_size - 1):
            pl.when(valid)(functools.partial(finish, zz))

    for layer in range(layers):
        total = jnp.sum(squares[layer], axis=0, keepdims=True)
        factor = magnitude_ref[pl.ds(layer, 1), :] / jnp.sqrt(total + epsilon)
        out_ref[layer] = (acc[layer] * factor).astype(out_ref.dtype)

    def drain(cond, make):
        when(cond, lambda: make().wait_send())

    for cond, make in pending:
        drain(cond, make)

    def sent(ref, sem):
        return pltpu.make_async_remote_copy(
            src_ref=ref, dst_ref=ref, send_sem=sem, recv_sem=arrive.at[0], device_id=partner, device_id_type=MESH
        )

    for r in range(1, rep_size):
        for valid, zz, step in sides(r):
            @pl.when(valid)
            def _(zz=zz, step=step):
                onward = (z + step >= 0) & (z + step <= rep_size - 1)
                for s in range(count):
                    for o in range(y_size):
                        yy = lax.rem(y + o, y_size)
                        at = (yy * rep_size + zz) * count + s
                        ref = piece(block(yy, c, zz), s)
                        sent(ref, csend.at[at]).wait_send()
                        if o == 0 or s == 0:
                            @pl.when(onward)
                            def _():
                                sent(ref, zsend.at[at]).wait_send()
                    if s > 0:
                        for o in range(1, y_size):
                            sent(
                                piece(block(y, c, zz), s), ysend.at[((o - 1) * rep_size + zz) * count + s]
                            ).wait_send()
    for o in range(1, y_size):
        yy = lax.rem(y + o, y_size)
        for s in range(1, count):
            sent(piece(block(yy, c, z), s), csend.at[(yy * rep_size + z) * count + s]).wait_send()


def local(sizes, prompts, frozen_projection_weight, lowrank_down_factor, lowrank_up_factor, magnitude):
    tp_size, dp_size, rep_size = sizes
    merged = merge_rows(frozen_projection_weight, lowrank_down_factor, lowrank_up_factor).astype(jnp.bfloat16)
    layers, rows, columns = merged.shape
    tokens = prompts.shape[0]
    blocks = dp_size * rep_size
    y_size = dp_size // 2
    count = 2 * layers
    dma = pltpu.SemaphoreType.DMA
    return pl.pallas_call(
        functools.partial(kernel, sizes),
        out_shape=jax.ShapeDtypeStruct((layers, tokens, columns), jnp.bfloat16),
        in_specs=[
            pl.BlockSpec(memory_space=pl.ANY),
            pl.BlockSpec(memory_space=pl.ANY),
            pl.BlockSpec(memory_space=pltpu.VMEM),
        ],
        out_specs=pl.BlockSpec(memory_space=pltpu.VMEM),
        scratch_shapes=[
            pltpu.VMEM((blocks, layers, rows, columns), jnp.bfloat16),
            pltpu.VMEM((blocks, tokens, rows), jnp.bfloat16),
            pltpu.VMEM((layers, tokens, columns), jnp.float32),
            pltpu.VMEM((layers, 8, columns), jnp.float32),
            dma((blocks * count,)),
            dma((y_size * rep_size * count,)),
            dma((y_size * count,)),
            dma((max(1, (y_size - 1) * rep_size * count),)),
            dma((y_size * rep_size * count,)),
            dma((max(1, (tp_size - 1) * blocks),)),
            dma((blocks,)),
            dma((blocks,)),
            dma(()),
        ],
        compiler_params=pltpu.CompilerParams(
            collective_id=0, has_side_effects=True, vmem_limit_bytes=66_000_000
        ),
        cost_estimate=pl.CostEstimate(
            flops=2 * layers * tokens * columns * rows * blocks, bytes_accessed=2 * blocks * rows * columns,
            transcendentals=0,
        ),
    )(prompts, merged, magnitude)


def solution(mesh):
    in_specs = (
        P(("dp", "rep"), "tp"),
        P(None, ("dp", "rep"), "tp"),
        P(None, ("dp", "rep"), None),
        P(None, None, "tp"),
        P(None, "tp"),
    )
    out_specs = P(None, ("dp", "rep"), "tp")
    sizes = tuple(mesh.shape[name] for name in ("tp", "dp", "rep"))
    return jax.shard_map(
        functools.partial(local, sizes), mesh=mesh, in_specs=in_specs, out_specs=out_specs, check_vma=False
    )
```

```python
import functools

import jax
import jax.numpy as jnp
from jax import lax
from jax.experimental import pallas as pl
from jax.experimental.pallas import tpu as pltpu
from jax.sharding import PartitionSpec as P

epsilon = 1e-06
MESH = pl.DeviceIdType.MESH


def merge_rows(weight_rows, down_rows, up_matrix):
    return weight_rows.astype(jnp.float32) + jnp.einsum(
        "lrk,lkc->lrc", down_rows, up_matrix, preferred_element_type=jnp.float32
    )


def kernel(
    sizes, prompts_ref, merged_ref, acc, squares,
    wbuf, pbuf,
    arrive, zsend, zown, ysend, csend, psend, parrive, load_p, load_w,
):
    tp_size, dp_size, rep_size = sizes
    y_size = dp_size // 2
    layers, rows, columns = merged_ref.shape
    groups = dp_size // tp_size
    x = lax.axis_index("tp")
    d = lax.axis_index("dp")
    z = lax.axis_index("rep")
    y, c = d // 2, lax.rem(d, 2)
    partner = {"tp": x, "dp": d + 1 - 2 * c, "rep": z}

    early = rows * 5 // 16
    pieces = [(0, 0, early), (0, early, rows - early)]
    for layer in range(1, layers):
        pieces += [(layer, 0, rows // 2), (layer, rows // 2, rows // 2)]
    count = len(pieces)

    def block(yy, cc, zz):
        return (yy * 2 + cc) * rep_size + zz

    def piece(b, s):
        layer, start, size = pieces[s]
        return wbuf.at[b, layer, pl.ds(start, size), :]

    pending = []

    def send(cond, ref, send_sem, recv_sem, device):
        def make():
            return pltpu.make_async_remote_copy(
                src_ref=ref, dst_ref=ref, send_sem=send_sem, recv_sem=recv_sem,
                device_id=device, device_id_type=MESH,
            )

        pending.append((cond, make))
        if cond is None:
            make().start()
        else:
            @pl.when(cond)
            def _():
                make().start()

    def wait_piece(b, s):
        pltpu.make_async_remote_copy(
            src_ref=piece(b, s), dst_ref=piece(b, s), send_sem=csend.at[0],
            recv_sem=arrive.at[b * count + s], device_id=partner, device_id_type=MESH,
        ).wait_recv()

    def z_device(step):
        return {"tp": x, "dp": d, "rep": z + step}

    def y_device(o):
        return {"tp": x, "dp": lax.rem(y + o, y_size) * 2 + c, "rep": z}

    def to_partner(cond, yy, zz, s):
        b = block(yy, c, zz)
        send(cond, piece(b, s), csend.at[(yy * rep_size + zz) * count + s], arrive.at[b * count + s], partner)

    def to_y(cond, zz, s):
        b = block(y, c, zz)
        for o in range(1, y_size):
            send(
                cond, piece(b, s), ysend.at[((o - 1) * rep_size + zz) * count + s],
                arrive.at[b * count + s], y_device(o),
            )

    def along_z(cond, yy, zz, s, step):
        b = block(yy, c, zz)
        send(
            cond, piece(b, s), zsend.at[(yy * rep_size + zz) * count + s],
            arrive.at[b * count + s], z_device(step),
        )

    def start_z(yy, s):
        b = block(yy, c, z)
        send(z < rep_size - 1, piece(b, s), zown.at[yy * count + s], arrive.at[b * count + s], z_device(1))
        along_z(z > 0, yy, z, s, -1)

    def when(cond, body):
        if cond is None:
            body()
        else:
            pl.when(cond)(body)

    me = block(y, c, z)
    load_weight = pltpu.make_async_copy(merged_ref, wbuf.at[me], load_w)
    load_weight.start()

    table = [sorted(range(rep_size), key=lambda k: (abs(k - at), k)) for at in range(rep_size)]

    def nearest(i):
        value = jnp.int32(table[0][i])
        for at in range(1, rep_size):
            value = jnp.where(z == at, jnp.int32(table[at][i]), value)
        return value

    own_chunks = []
    for i in range(rep_size):
        for g in range(groups):
            own_chunks.append((g * rep_size + nearest(i), x * groups * rep_size + g * rep_size + nearest(i)))

    def load_chunk(j, b):
        start = pl.multiple_of(j * rows, rows)
        return pltpu.make_async_copy(prompts_ref.at[:, pl.ds(start, rows)], pbuf.at[b], load_p.at[b])

    for j, b in own_chunks:
        load_chunk(j, b).start()

    barrier = pltpu.get_barrier_semaphore()
    pl.semaphore_signal(barrier, 1, device_id=partner, device_id_type=MESH)
    for o in range(1, y_size):
        pl.semaphore_signal(barrier, 1, device_id=y_device(o), device_id_type=MESH)
    for o in range(1, tp_size):
        pl.semaphore_signal(
            barrier, 1, device_id={"tp": lax.rem(x + o, tp_size), "dp": d, "rep": z}, device_id_type=MESH
        )

    @pl.when(z > 0)
    def _():
        pl.semaphore_signal(barrier, 1, device_id=z_device(-1), device_id_type=MESH)

    @pl.when(z < rep_size - 1)
    def _():
        pl.semaphore_signal(barrier, 1, device_id=z_device(1), device_id_type=MESH)

    neighbours = jnp.where(z > 0, 1, 0) + jnp.where(z < rep_size - 1, 1, 0)
    pl.semaphore_wait(barrier, neighbours + (1 + y_size - 1 + tp_size - 1))

    load_weight.wait()
    for s in range(count):
        to_y(None, z, s)
        start_z(y, s)
    for j, b in own_chunks:
        load_chunk(j, b).wait()
        for o in range(1, tp_size):
            send(
                None, pbuf.at[b], psend.at[(o - 1) * dp_size * rep_size + b], parrive.at[b],
                {"tp": lax.rem(x + o, tp_size), "dp": d, "rep": z},
            )
    for s in range(count):
        to_partner(None, y, z, s)

    acc[...] = jnp.zeros_like(acc)
    squares[...] = jnp.zeros_like(squares)
    tile = min(256, columns)

    def wait_chunk(b):
        @pl.when(b // (groups * rep_size) != x)
        def _():
            pltpu.make_async_remote_copy(
                src_ref=pbuf.at[b], dst_ref=pbuf.at[b], send_sem=psend.at[0], recv_sem=parrive.at[b],
                device_id=partner, device_id_type=MESH,
            ).wait_recv()

    def compute(b, first, last):
        tiles = columns // tile

        def step(t, carry):
            layer = first + t // tiles
            at = pl.ds(pl.multiple_of(lax.rem(t, tiles) * tile, tile), tile)
            weight = wbuf[b, layer, :, at]
            acc[layer, :, at] += jnp.dot(pbuf[b], weight, preferred_element_type=jnp.float32)
            wide = weight.astype(jnp.float32)
            squares[layer, :, at] += jnp.sum((wide * wide).reshape(rows // 8, 8, tile), axis=0)
            return carry

        lax.fori_loop(0, (last - first) * tiles, step, 0)

    def held(layer):
        return [s for s in range(count) if pieces[s][0] == layer]

    def own_layer(zz, layer):
        mine, other = block(y, c, zz), block(y, 1 - c, zz)
        if layer == 0:
            wait_chunk(mine)
        compute(mine, layer, layer + 1)
        for s in held(layer):
            wait_piece(other, s)
        if layer == 0:
            wait_chunk(other)
        compute(other, layer, layer + 1)

    def own(zz):
        mine, other = block(y, c, zz), block(y, 1 - c, zz)
        wait_chunk(mine)
        compute(mine, 0, layers)
        for s in range(count):
            wait_piece(other, s)
        wait_chunk(other)
        compute(other, 0, layers)

    def across(zz):
        for o in range(1, y_size):
            yy = lax.rem(y + o, y_size)
            mine, other = block(yy, c, zz), block(yy, 1 - c, zz)
            for layer in range(layers):
                for s in held(layer):
                    if s > 0:
                        wait_piece(mine, s)
                        to_partner_plain(yy, zz, s)
                if layer == 0:
                    wait_chunk(mine)
                compute(mine, layer, layer + 1)
                for s in held(layer):
                    wait_piece(other, s)
                if layer == 0:
                    wait_chunk(other)
                compute(other, layer, layer + 1)

    def to_partner_plain(yy, zz, s):
        b = block(yy, c, zz)

        def make():
            return pltpu.make_async_remote_copy(
                src_ref=piece(b, s), dst_ref=piece(b, s), send_sem=csend.at[(yy * rep_size + zz) * count + s],
                recv_sem=arrive.at[b * count + s], device_id=partner, device_id_type=MESH,
            )

        make().start()

    def take(zz, s, step):
        onward = (z + step >= 0) & (z + step <= rep_size - 1)

        def arrived(yy):
            b = block(yy, c, zz)
            wait_piece(b, s)

            @pl.when(onward)
            def _():
                pltpu.make_async_remote_copy(
                    src_ref=piece(b, s), dst_ref=piece(b, s), send_sem=zsend.at[(yy * rep_size + zz) * count + s],
                    recv_sem=arrive.at[b * count + s], device_id=z_device(step), device_id_type=MESH,
                ).start()

        arrived(y)
        if s > 0:
            b = block(y, c, zz)
            for o in range(1, y_size):
                pltpu.make_async_remote_copy(
                    src_ref=piece(b, s), dst_ref=piece(b, s),
                    send_sem=ysend.at[((o - 1) * rep_size + zz) * count + s],
                    recv_sem=arrive.at[b * count + s], device_id=y_device(o), device_id_type=MESH,
                ).start()
        to_partner_plain(y, zz, s)
        if s == 0:
            for o in range(1, y_size):
                yy = lax.rem(y + o, y_size)
                arrived(yy)
                to_partner_plain(yy, zz, 0)

    for o in range(1, y_size):
        yy = lax.rem(y + o, y_size)
        wait_piece(block(yy, c, z), 0)
        start_z(yy, 0)
        to_partner(None, yy, z, 0)

    def sides(r):
        return ((z - r >= 0, z - r, 1), (z + r <= rep_size - 1, z + r, -1))

    far = jnp.maximum(z, rep_size - 1 - z)

    def each(r, cond, body):
        def run():
            if 2 * r <= rep_size - 1:
                for valid, zz, step in sides(r):
                    pl.when(valid)(functools.partial(body, zz, step))
            else:
                low = z - r >= 0
                body(jnp.where(low, z - r, z + r), jnp.where(low, 1, -1))

        pl.when(cond & (r <= far))(run)

    def take_all(r, some):
        for s in some:
            each(r, r <= far, lambda zz, step, s=s: take(zz, s, step))

    if rep_size > 1:
        take_all(1, range(count))
    own(z)
    across(z)
    if rep_size > 1:
        each(1, far == 1, lambda zz, step: own(zz))
    for r in range(2, rep_size):
        two = (z - (r - 1) >= 0) & (z + (r - 1) <= rep_size - 1)
        one = jnp.logical_not(two) & (r <= far)
        last = r == far
        take_all(r, range(2))
        each(r - 1, one, lambda zz, step: own(zz))
        take_all(r, range(2, count - 1))
        each(r - 1, one, lambda zz, step: across(zz))
        each(r, one & last, lambda zz, step: own_layer(zz, 0))
        take_all(r, range(count - 1, count))

        def rest(zz, step):
            for layer in range(1, layers):
                own_layer(zz, layer)

        each(r, one & last, rest)
        if 2 * (r - 1) <= rep_size - 1:
            both = two & (r <= far)
            each(r - 1, both, lambda zz, step: own(zz))
            each(r, both & last, lambda zz, step: own(zz))
            each(r - 1, both, lambda zz, step: across(zz))
    for r in range(1, rep_size):
        if any(max(at, rep_size - 1 - at) == r for at in range(rep_size)):
            each(r, far == r, lambda zz, step: across(zz))

    def drain(cond, make):
        when(cond, lambda: make().wait_send())

    for cond, make in pending:
        drain(cond, make)

    def sent(ref, sem):
        return pltpu.make_async_remote_copy(
            src_ref=ref, dst_ref=ref, send_sem=sem, recv_sem=arrive.at[0], device_id=partner, device_id_type=MESH
        )

    for r in range(1, rep_size):
        for valid, zz, step in sides(r):
            @pl.when(valid)
            def _(zz=zz, step=step):
                onward = (z + step >= 0) & (z + step <= rep_size - 1)
                for s in range(count):
                    for o in range(y_size):
                        yy = lax.rem(y + o, y_size)
                        at = (yy * rep_size + zz) * count + s
                        ref = piece(block(yy, c, zz), s)
                        sent(ref, csend.at[at]).wait_send()
                        if o == 0 or s == 0:
                            @pl.when(onward)
                            def _():
                                sent(ref, zsend.at[at]).wait_send()
                    if s > 0:
                        for o in range(1, y_size):
                            sent(
                                piece(block(y, c, zz), s), ysend.at[((o - 1) * rep_size + zz) * count + s]
                            ).wait_send()
    for o in range(1, y_size):
        yy = lax.rem(y + o, y_size)
        for s in range(1, count):
            sent(piece(block(yy, c, z), s), csend.at[(yy * rep_size + z) * count + s]).wait_send()


def local(sizes, prompts, frozen_projection_weight, lowrank_down_factor, lowrank_up_factor, magnitude):
    tp_size, dp_size, rep_size = sizes
    merged = merge_rows(frozen_projection_weight, lowrank_down_factor, lowrank_up_factor).astype(jnp.bfloat16)
    layers, rows, columns = merged.shape
    tokens = prompts.shape[0]
    blocks = dp_size * rep_size
    y_size = dp_size // 2
    count = 2 * layers
    dma = pltpu.SemaphoreType.DMA
    product, squares = pl.pallas_call(
        functools.partial(kernel, sizes),
        out_shape=(
            jax.ShapeDtypeStruct((layers, tokens, columns), jnp.float32),
            jax.ShapeDtypeStruct((layers, 8, columns), jnp.float32),
        ),
        in_specs=[
            pl.BlockSpec(memory_space=pl.ANY),
            pl.BlockSpec(memory_space=pl.ANY),
        ],
        out_specs=(pl.BlockSpec(memory_space=pltpu.VMEM), pl.BlockSpec(memory_space=pltpu.VMEM)),
        scratch_shapes=[
            pltpu.VMEM((blocks, layers, rows, columns), jnp.bfloat16),
            pltpu.VMEM((blocks, tokens, rows), jnp.bfloat16),
            dma((blocks * count,)),
            dma((y_size * rep_size * count,)),
            dma((y_size * count,)),
            dma((max(1, (y_size - 1) * rep_size * count),)),
            dma((y_size * rep_size * count,)),
            dma((max(1, (tp_size - 1) * blocks),)),
            dma((blocks,)),
            dma((blocks,)),
            dma(()),
        ],
        compiler_params=pltpu.CompilerParams(
            collective_id=0, has_side_effects=True, vmem_limit_bytes=66_000_000
        ),
        cost_estimate=pl.CostEstimate(
            flops=2 * layers * tokens * columns * rows * blocks, bytes_accessed=2 * blocks * rows * columns,
            transcendentals=0,
        ),
    )(prompts, merged)
    factor = magnitude / jnp.sqrt(jnp.sum(squares, axis=1) + epsilon)
    return (product * factor[:, None, :]).astype(jnp.bfloat16)


def solution(mesh):
    in_specs = (
        P(("dp", "rep"), "tp"),
        P(None, ("dp", "rep"), "tp"),
        P(None, ("dp", "rep"), None),
        P(None, None, "tp"),
        P(None, "tp"),
    )
    out_specs = P(None, ("dp", "rep"), "tp")
    sizes = tuple(mesh.shape[name] for name in ("tp", "dp", "rep"))
    return jax.shard_map(
        functools.partial(local, sizes), mesh=mesh, in_specs=in_specs, out_specs=out_specs, check_vma=False
    )
```
